256 devices in a mesh: sample: 16 (over y_hi, x, core), line: 16 (over z, y_lo).
Axes of the slice: x: 4, y: 4 (y_hi: 2, y_lo: 2; y = y_hi * 2 + y_lo), z: 8, core: 2. Of those that a mesh axis runs over, the one named last changes fastest.
Arguments:
- wind_dev: bfloat16 [8192, 10000], P('sample', 'line'), may hold values from -6 to 6
- ptdf: bfloat16 [4096, 10000], P('line'), may hold values from -0.0625 to 0.0625
- region_weights: bfloat16 [31, 10000], replicated, may hold values from -0.0625 to 0.0625
- incidence: int32 [12706, 2], replicated, may hold values from 0 to 9999
- monitored: int32 [4096], P('line'), may hold values from 0 to 12705
- ratings: float32 [12706], replicated, may hold values from 1 to 3
- base_flow: float32 [4096], P('line'), may hold values from -6 to 6
- line_cost: float32 [4096], P('line'), may hold values from 0.2 to 20
- policy: float32 [32, 4096], P(None, 'line'), may hold values from -0.6 to 0.6
Outputs:
- new_policy: float32 [32, 4096], P(None, 'line')
- new_flows: float32 [8192, 4096], P('sample', 'line')
- decrement: float32 [], replicated
- grad_norm: float32 [], replicated
The draws below stay inside these ranges and needn't reach their ends.
All inputs are finite; a program needn't handle non-finite values.
Results may differ from the reference program's by a relative error of at most 0.0003.
Values may be sent and summed in bfloat16 or wider, within the bound.
No kernel may reach another device: no remote copies, remote signals or barrier semaphores. Data moves between devices by JAX's collectives and lax.ppermute only.
A program may use at most 128 MiB of HBM per device.

```python
import math
import jax
import jax.numpy as jnp
from jax import lax

NUM_BUSES = 10000
MONITORED = 4096
GRID_LINES = 12706
REGIONS = 31
FEATURES = 32
SCENARIOS = 8192


def draw_line_cost(key, part):
    position = jnp.arange(MONITORED, dtype=jnp.float32) / MONITORED
    low_end = 0.3
    high_end = 3.0
    rise_rate = 1.1
    uniform_draw = jax.random.uniform(key, (MONITORED,), jnp.float32)
    spread_term = jnp.exp(jnp.log(low_end) + uniform_draw * (jnp.log(high_end) - jnp.log(low_end)))
    return spread_term * jnp.exp(rise_rate * position)


def with_ends(drawn, rng, low, high):
    longest = drawn.shape.index(max(drawn.shape))
    spots = []
    for shift in (0, 1):
        where = [jax.random.randint(jax.random.fold_in(rng, axis), (), 0, length) for axis, length in enumerate(drawn.shape)]
        where[longest] = (where[longest] + shift) % drawn.shape[longest]
        spots.append(tuple(where))
    return drawn.at[spots[0]].set(low).at[spots[1]].set(high)


def steps_of(own_key, extent, cuts, low, largest):
    loudness, own = 1.0, jax.random.fold_in(own_key, 6)
    for dim, parts in cuts:
        steps = jnp.exp(jax.random.uniform(jax.random.fold_in(own, dim), (parts,), jnp.float32, low / len(cuts), largest / len(cuts)))
        loudness = loudness * jnp.repeat(steps, extent[dim] // parts).reshape([-1 if axis == dim else 1 for axis in range(len(extent))])
    return loudness


def noise(stream_key, dims, scale, reach, shards=(), held_as=jnp.bfloat16):
    result = jax.random.normal(stream_key, dims, jnp.float32) * scale
    if len(shards) > 0:
        result = steps_of(stream_key, dims, shards, -0.22, 0.18) * result
    return jnp.clip(result, min=-reach, max=reach).astype(held_as)


def setup_inputs(seed: int = 0) -> dict:
    key_of = jax.random.split(jax.random.key(seed), 10)
    return {
        "wind_dev": noise(key_of[0], (SCENARIOS, NUM_BUSES), 1.0, 6.0, ((0, 16), (1, 16))),
        "ptdf": noise(key_of[1], (MONITORED, NUM_BUSES), NUM_BUSES ** -0.5, 0.0625, ((0, 16),)),
        "region_weights": noise(key_of[2], (REGIONS, NUM_BUSES), NUM_BUSES ** -0.5, 0.0625),
        "incidence": with_ends(jax.random.randint(key_of[3], (GRID_LINES, 2), 0, NUM_BUSES), jax.random.fold_in(key_of[3], 1), 0, NUM_BUSES - 1).astype(jnp.int32),
        "monitored": with_ends(jax.random.randint(key_of[4], (MONITORED,), 0, GRID_LINES), jax.random.fold_in(key_of[4], 1), 0, GRID_LINES - 1).astype(jnp.int32),
        "ratings": jnp.clip(jnp.exp(jax.random.uniform(key_of[5], (GRID_LINES,), jnp.float32, math.log(1.0), math.log(3.0))), 1.0, 3.0),
        "base_flow": noise(key_of[6], (MONITORED,), 1.0, 6.0, ((0, 16),), jnp.float32),
        "line_cost": draw_line_cost(jax.random.fold_in(key_of[9], 71), 0),
        "policy": jnp.clip(jax.random.uniform(key_of[8], (FEATURES, MONITORED), jnp.float32, -0.6, 0.6) * steps_of(key_of[8], (FEATURES, MONITORED), ((1, 16),), -0.4, 0.0), -0.6, 0.6),
    }


ridge_weight = 1.0
barrier_weight = 0.1
smoothing = 0.5

def penalty_terms(factors, ends_diff, slope_term, curve_term, weight):
    highest = lax.Precision.HIGHEST
    regions = factors.shape[1]
    lines_here = slope_term.shape[1]
    outer_prod = (factors[:, :, None] * factors[:, None, :]).reshape(factors.shape[0], regions * regions)
    block_rr = lax.dot_general(outer_prod, curve_term, (((0,), (0,)), ((), ())), precision=highest)
    weighted = curve_term * ends_diff
    cross_re = lax.dot_general(factors, weighted, (((0,), (0,)), ((), ())), precision=highest)
    corner = lax.optimization_barrier(jnp.sum(weighted * ends_diff, axis=0))
    upper_rows = jnp.concatenate([block_rr.reshape(regions, regions, lines_here), cross_re[:, None, :]], axis=1)
    bottom = jnp.concatenate([cross_re[None, :, :], corner[None, None, :]], axis=1)
    hessian = jnp.concatenate([upper_rows, bottom], axis=0) * weight
    grad_rr = lax.dot_general(factors, slope_term, (((0,), (0,)), ((), ())), precision=highest)
    gradient = jnp.concatenate([grad_rr, lax.optimization_barrier(jnp.sum(slope_term * ends_diff, axis=0))[None, :]], axis=0) * weight
    return (hessian.reshape((regions + 1) * (regions + 1), lines_here), gradient)

def factor_solve(hessian, gradient):
    features = gradient.shape[0]
    positions = jnp.arange(features, dtype=jnp.int32)

    def chol_column(column, lower_tri):
        target = lax.dynamic_index_in_dim(hessian, column, 1, keepdims=False)
        row_here = lax.dynamic_index_in_dim(lower_tri, column, 0, keepdims=False)
        running = target - lax.optimization_barrier(jnp.sum(lower_tri * row_here[None, :, :], axis=1))
        pivot_val = jnp.sqrt(lax.dynamic_index_in_dim(running, column, 0, keepdims=False))
        new_col = jnp.where((positions >= column)[:, None], running / pivot_val[None, :], jnp.zeros_like(running))
        select = (positions == column).astype(hessian.dtype)
        return lower_tri + new_col[:, None, :] * select[None, :, None]
    lower_tri = lax.fori_loop(0, features, chol_column, jnp.zeros_like(hessian))

    def forward_row(row_index, forward):
        row_here = lax.dynamic_index_in_dim(lower_tri, row_index, 0, keepdims=False)
        running = lax.dynamic_index_in_dim(gradient, row_index, 0, keepdims=False) - lax.optimization_barrier(jnp.sum(row_here * forward, axis=0))
        value = running / lax.dynamic_index_in_dim(row_here, row_index, 0, keepdims=False)
        select = (positions == row_index).astype(gradient.dtype)
        return forward + select[:, None] * value[None, :]
    forward = lax.fori_loop(0, features, forward_row, jnp.zeros_like(gradient))

    def backward_row(turn, backward):
        row_index = features - 1 - turn
        col_here = lax.dynamic_index_in_dim(lower_tri, row_index, 1, keepdims=False)
        running = lax.dynamic_index_in_dim(forward, row_index, 0, keepdims=False) - lax.optimization_barrier(jnp.sum(col_here * backward, axis=0))
        value = running / lax.dynamic_index_in_dim(col_here, row_index, 0, keepdims=False)
        select = (positions == row_index).astype(gradient.dtype)
        return backward + select[:, None] * value[None, :]
    backward = lax.fori_loop(0, features, backward_row, jnp.zeros_like(gradient))
    return (forward, -backward)

def owner_step(hessian_flat, gradient, policy_part):
    features = gradient.shape[0]
    lines_here = gradient.shape[1]
    hessian = hessian_flat.reshape(features, features, lines_here)
    margin_sq = 1.0 - policy_part * policy_part
    diag_terms = ridge_weight + barrier_weight * 2.0 * (1.0 + policy_part * policy_part) / (margin_sq * margin_sq)
    hessian = hessian + jnp.eye(features, dtype=hessian.dtype)[:, :, None] * diag_terms[:, None, :]
    gradient = gradient + ridge_weight * policy_part + barrier_weight * 2.0 * policy_part / margin_sq
    forward, newton_step = factor_solve(hessian, gradient)
    return (gradient, forward, newton_step)

def reference(wind_dev, ptdf, region_weights, incidence, monitored, ratings, base_flow, line_cost, policy):
    highest = lax.Precision.HIGHEST
    regions = region_weights.shape[0]
    endpoints = jnp.take(incidence, monitored, axis=0)
    from_bus = endpoints[:, 0]
    to_bus = endpoints[:, 1]
    rating = jnp.take(ratings, monitored)
    total_scen = wind_dev.shape[0]
    grid_flow = jnp.dot(wind_dev, ptdf.T, preferred_element_type=jnp.float32)
    factors = jnp.dot(wind_dev, region_weights.T, preferred_element_type=jnp.float32)
    ends_diff = jnp.take(wind_dev, to_bus, axis=1).astype(jnp.float32) - jnp.take(wind_dev, from_bus, axis=1).astype(jnp.float32)
    line_flow = grid_flow + base_flow[None, :] + jnp.dot(factors, policy[:regions], precision=highest) + policy[regions][None, :] * ends_diff
    prob_up = jax.nn.sigmoid((line_flow - rating[None, :]) / smoothing)
    prob_down = jax.nn.sigmoid((-line_flow - rating[None, :]) / smoothing)
    slope_term = prob_up - prob_down
    curve_term = (prob_up * (1.0 - prob_up) + prob_down * (1.0 - prob_down)) / smoothing
    weight = line_cost / total_scen
    hessian_sum, gradient_sum = penalty_terms(factors, ends_diff, slope_term, curve_term, weight)
    gradient, forward, newton_step = owner_step(hessian_sum, gradient_sum, policy)
    decrement_sq = jnp.sum(forward * forward)
    norm_sq = jnp.sum(gradient * gradient)
    features = policy.shape[0]
    step_length = 1.0 / (1.0 + jnp.sqrt(decrement_sq / (barrier_weight * features * MONITORED)))
    new_policy = policy + step_length * newton_step
    shift_flow = jnp.dot(factors, newton_step[:regions], precision=highest) + newton_step[regions][None, :] * ends_diff
    new_flows = line_flow + step_length * shift_flow
    return (new_policy, new_flows, jnp.sqrt(decrement_sq), jnp.sqrt(norm_sq))
```

```python
import functools

import jax
import jax.numpy as jnp
from jax import lax
from jax.experimental import pallas as pl
from jax.experimental.pallas import tpu as pltpu
from jax.sharding import Mesh
from jax.sharding import PartitionSpec as P

LINE = ("line_0", "line_1")
SAMPLE = ("sample_0", "sample_1", "sample_2")


ridge_weight = 1.0
barrier_weight = 0.1
smoothing = 0.5

HIGHEST = lax.Precision.HIGHEST
F32 = jnp.float32
BF16 = jnp.bfloat16
NT = (((1,), (1,)), ((), ()))
CHUNK = 256
AHEAD = 2
MIB = 1 << 20


def row_blocks(a):
    return a // 8 + 1


def row_starts(features):
    starts, at = [], 0
    for a in range(features):
        starts.append(at)
        at += 8 * row_blocks(a)
    return starts, at


def kernel_params(vmem_mib):
    return pltpu.CompilerParams(vmem_limit_bytes=vmem_mib * MIB)


def cost(flops, nbytes):
    return pl.CostEstimate(flops=int(flops), bytes_accessed=int(nbytes), transcendentals=0)


def repack_kernel(width, padded, turned, meta, rows_ref, out_ref):
    lines, total = out_ref.shape
    for parity in (0, 1):

        @pl.when(meta[0] == parity)
        def _():
            for b in range(total // padded):
                start, at = width * (2 * b + parity), b * padded
                tail = at + width // 128 * 128
                out_ref[:, tail : at + padded] = jnp.zeros(
                    (lines, at + padded - tail), out_ref.dtype
                )
                if turned:
                    low = start // 16 * 16
                    first = pl.multiple_of(meta[1] * lines, lines)
                    window = rows_ref[low : low + padded, pl.ds(first, lines)].T
                    out_ref[:, at : at + width] = window[:, start - low : start - low + width]
                else:
                    out_ref[:, at : at + width] = rows_ref[:, start : start + width]


def repack(rows, turned, parity, first, lines, blocks, width, padded):
    meta = jnp.stack([parity, jnp.int32(first)]).astype(jnp.int32)
    if turned:
        assert all(width * b % 16 + width <= padded for b in range(2 * blocks))
        assert all(width * b // 16 * 16 + padded <= rows.shape[0] for b in range(2 * blocks))
    return pl.pallas_call(
        functools.partial(repack_kernel, width, padded, turned),
        grid_spec=pltpu.PrefetchScalarGridSpec(
            num_scalar_prefetch=1,
            in_specs=[pl.BlockSpec(memory_space=pltpu.VMEM)],
            out_specs=pl.BlockSpec(memory_space=pltpu.VMEM),
        ),
        out_shape=jax.ShapeDtypeStruct((lines, blocks * padded), rows.dtype),
        compiler_params=kernel_params(24),
        cost_estimate=cost(3e9, 2 * rows.size),
        name="repack",
    )(meta, rows)


def ends_kernel(width, padded, meta, ids_ref, out_ref):
    lines, total = out_ref.shape
    lane = lax.broadcasted_iota(jnp.int32, (lines, padded), 1)
    lane = jnp.where(lane < width, lane, -1)
    for b in range(total // padded):
        base = width * (2 * b + meta[0])
        first, last = ids_ref[:, 0:1] - base, ids_ref[:, 1:2] - base
        first = jnp.where(first < 0, -2, first)
        last = jnp.where(last < 0, -2, last)
        hits = jnp.where(lane == last, 1.0, 0.0) - jnp.where(lane == first, 1.0, 0.0)
        out_ref[:, b * padded : (b + 1) * padded] = hits.astype(out_ref.dtype)


def ends_blocks(ids, parity, blocks, width, padded):
    lines = ids.shape[0]
    return pl.pallas_call(
        functools.partial(ends_kernel, width, padded),
        grid_spec=pltpu.PrefetchScalarGridSpec(
            num_scalar_prefetch=1,
            in_specs=[pl.BlockSpec(memory_space=pltpu.VMEM)],
            out_specs=pl.BlockSpec(memory_space=pltpu.VMEM),
        ),
        out_shape=jax.ShapeDtypeStruct((lines, blocks * padded), BF16),
        compiler_params=kernel_params(16),
        cost_estimate=cost(3e9, 2 * blocks * lines * padded),
        name="ends",
    )(jnp.stack([parity]).astype(jnp.int32), ids)


def flows_kernel(n, padded, meta, *refs):
    pieces, rhs, (own_ref, send_ref, held) = refs[:n], refs[n : n + 6], refs[n + 6 :]
    ptdf_ref, ends_ref, region_ref, part_a_ref, part_b_ref, part_ends_ref = rhs
    width = pieces[0].shape[0]
    lines = ptdf_ref.shape[0]
    even = width // 16 * 16
    for j in range(n):
        at = pl.multiple_of(meta[j] * padded, padded)
        held[pl.ds(at + even, padded - even)] = jnp.zeros((padded - even, held.shape[1]), held.dtype)
        held[pl.ds(at, even)] = pieces[j][0:even]
        held[pl.ds(at + even, width - even)] = pieces[j][even:width]

    def times(x):
        return jnp.dot(x[...], held[...], preferred_element_type=F32)

    half = lines // 2
    first = pl.multiple_of(meta[n] * half, half)
    second = pl.multiple_of((1 - meta[n]) * half, half)
    send_ref[pl.ds(first, half)] = times(part_a_ref)
    send_ref[pl.ds(second, half)] = times(part_b_ref)
    send_ref[lines : 2 * lines] = times(part_ends_ref)
    factors = times(region_ref)
    send_ref[2 * lines :] = factors
    own_ref[2 * lines :] = factors
    own_ref[0:lines] = times(ptdf_ref)
    own_ref[lines : 2 * lines] = times(ends_ref)


def partial_flows(meta, pieces, rhs, padded):
    n = len(pieces)
    chunk = pieces[0].shape[1]
    total = 2 * rhs[0].shape[0] + rhs[2].shape[0]
    whole = pl.BlockSpec(memory_space=pltpu.VMEM)
    out = jax.ShapeDtypeStruct((total, chunk), F32)
    return pl.pallas_call(
        functools.partial(flows_kernel, n, padded),
        grid_spec=pltpu.PrefetchScalarGridSpec(
            num_scalar_prefetch=1,
            in_specs=[whole] * (n + len(rhs)),
            out_specs=[whole, whole],
            scratch_shapes=[pltpu.VMEM((n * padded, chunk), BF16)],
        ),
        out_shape=[out, out],
        compiler_params=kernel_params(28),
        cost_estimate=cost(6e9, n * 4 * padded * total),
        name="flows",
    )(meta, *pieces, *rhs)


def sigmoid(x):
    return 1.0 / (1.0 + jnp.exp(-x))


def penalty_kernel(has_prev, own_ref, got_ref, line_ref, policy_ref, *refs):
    prev_ref = refs[0] if has_prev else None
    flow_ref, ends_ref, factor_ref, sums_ref = refs[1 if has_prev else 0 :]
    lines = flow_ref.shape[0]
    feats, chunk = factor_ref.shape
    both = own_ref[...] + got_ref[...]
    grid_flow, ends, factors = both[0:lines], both[lines : 2 * lines], both[2 * lines :]
    policy = policy_ref[...]
    flow = (
        grid_flow
        + line_ref[:, 0:1]
        + jnp.dot(policy, factors, precision=HIGHEST, preferred_element_type=F32)
        + policy[:, feats - 1 : feats] * ends
    )
    rating = line_ref[:, 1:2]
    up = sigmoid((flow - rating) / smoothing)
    down = sigmoid((-flow - rating) / smoothing)
    slope = up - down
    curve = (up * (1.0 - up) + down * (1.0 - down)) / smoothing
    weighted = curve * ends
    rows = [factors[0 : 8 * row_blocks(a)] * factors[a : a + 1] for a in range(feats - 1)]
    count = sum(r.shape[0] for r in rows)
    products = jnp.concatenate(rows + [jnp.zeros((feats, chunk), F32)], axis=0)
    lifted = jnp.concatenate([jnp.zeros((count, chunk), F32), factors], axis=0)
    curved = lax.dot_general(
        jnp.concatenate([curve, weighted], axis=1),
        jnp.concatenate([products, lifted], axis=1),
        NT,
        precision=HIGHEST,
        preferred_element_type=F32,
    )
    pad = jnp.zeros((128 - feats, chunk), F32)
    sloped = lax.dot_general(
        slope,
        jnp.concatenate([factors, pad], axis=0),
        NT,
        precision=HIGHEST,
        preferred_element_type=F32,
    )
    size = count + feats
    corner = jnp.sum(weighted * ends, axis=1, keepdims=True)
    last = jnp.sum(slope * ends, axis=1, keepdims=True)
    col = lax.broadcasted_iota(jnp.int32, (lines, size), 1)
    curved = curved + jnp.where(col == size - 1, corner, 0.0)
    col = lax.broadcasted_iota(jnp.int32, (lines, 128), 1)
    sloped = sloped + jnp.where(col == feats - 1, last, 0.0)
    if has_prev:
        curved = curved + prev_ref[:, 0:size]
        sloped = sloped + prev_ref[:, size:]
    sums_ref[:, 0:size] = curved
    sums_ref[:, size:] = sloped
    flow_ref[...] = flow
    ends_ref[...] = ends
    factor_ref[...] = factors


def penalty(own, got, per_line, policy_t, prev):
    lines, feats = policy_t.shape
    chunk = own.shape[1]
    size = row_starts(feats)[1] + 128
    args = [own, got, per_line, policy_t] + ([] if prev is None else [prev])
    return pl.pallas_call(
        functools.partial(penalty_kernel, prev is not None),
        out_shape=[
            jax.ShapeDtypeStruct((lines, chunk), F32),
            jax.ShapeDtypeStruct((lines, chunk), F32),
            jax.ShapeDtypeStruct((feats, chunk), F32),
            jax.ShapeDtypeStruct((lines, size), F32),
        ],
        compiler_params=kernel_params(24),
        cost_estimate=cost(3e9, 4 * lines * (size * 2 + chunk * 6)),
        name="penalty",
    )(*args)


def solve_kernel(copies, lines, sums_ref, weight_ref, policy_ref, out_ref, rows_ref):
    feats = policy_ref.shape[0]
    starts, size = row_starts(feats)
    total = sums_ref[0:lines]
    for src in range(1, copies):
        total = total + sums_ref[src * lines : (src + 1) * lines]
    square = jnp.concatenate([total, jnp.zeros((128 - lines, total.shape[1]), F32)], axis=0)
    weight = weight_ref[0:1]
    policy = policy_ref[...]
    margin = 1.0 - policy * policy
    diag = ridge_weight + barrier_weight * 2.0 * (1.0 + policy * policy) / (margin * margin)
    rows_ref[...] = square.T * weight
    g = (
        rows_ref[size : size + feats]
        + ridge_weight * policy
        + barrier_weight * 2.0 * policy / margin
    )
    norm = jnp.sum(g * g, axis=0, keepdims=True)
    sub = lax.broadcasted_iota(jnp.int32, (8, 128), 0)
    row = lax.broadcasted_iota(jnp.int32, (feats, 128), 0)
    for a in range(feats):
        at = starts[a] + 8 * (a // 8)
        rows_ref[at : at + 8] += jnp.where(sub == a % 8, diag[a : a + 1], 0.0)
    decrement = jnp.zeros((1, 128), F32)
    inverses = [None] * feats
    for c in reversed(range(feats)):
        height = 8 * row_blocks(c)
        pivot = rows_ref[starts[c] : starts[c] + height]
        inverse = 1.0 / pivot[c : c + 1]
        inverses[c] = inverse
        g_c = g[c : c + 1]
        decrement = decrement + g_c * g_c * inverse
        scaled = pivot * inverse
        for i in range(c):
            tall = 8 * row_blocks(i)
            rows_ref[starts[i] : starts[i] + tall] -= scaled[i : i + 1] * pivot[0:tall]
        full = scaled
        if height < feats:
            full = jnp.concatenate([scaled, jnp.zeros((feats - height, 128), F32)], axis=0)
        g = g - jnp.where(row < c, full * g_c, 0.0)
    x = jnp.zeros((feats, 128), F32)
    for i in range(feats):
        height = 8 * row_blocks(i)
        known = jnp.sum(
            rows_ref[starts[i] : starts[i] + height] * x[0:height], axis=0, keepdims=True
        )
        x_i = (g[i : i + 1] - known) * inverses[i]
        x = jnp.where(row == i, x_i, x)
    tail = jnp.concatenate([decrement, norm, jnp.zeros((128 - feats - 2, 128), F32)], axis=0)
    result = jnp.concatenate([-x, tail], axis=0).T[0:lines]
    for dst in range(copies):
        out_ref[dst * lines : (dst + 1) * lines] = result


def solve(sums, weight, policy_part, copies):
    lines = sums.shape[0] // copies
    return pl.pallas_call(
        functools.partial(solve_kernel, copies, lines),
        out_shape=jax.ShapeDtypeStruct((copies * lines, 128), F32),
        scratch_shapes=[pltpu.VMEM((sums.shape[1], 128), F32)],
        compiler_params=kernel_params(16),
        cost_estimate=cost(1e9, 4 * sums.size),
        name="solve",
    )(sums, weight, policy_part)


def tally_kernel(step_ref, out_ref):
    out_ref[...] = jnp.broadcast_to(jnp.sum(step_ref[...], axis=0, keepdims=True), out_ref.shape)


def tally(step, groups):
    return pl.pallas_call(
        tally_kernel,
        out_shape=jax.ShapeDtypeStruct((8 * groups, 128), F32),
        compiler_params=kernel_params(8),
        name="tally",
    )(step)


def shift_kernel(n, step_ref, *refs):
    flows, ends, factors = refs[:n], refs[n : 2 * n], refs[2 * n : 3 * n]
    flow_ref, shift_ref = refs[3 * n :]
    feats, chunk = factors[0].shape
    step = step_ref[...]
    for j in range(n):
        shift = (
            jnp.dot(step[:, 0:feats], factors[j][...], precision=HIGHEST, preferred_element_type=F32)
            + step[:, feats - 1 : feats] * ends[j][...]
        )
        shift_ref[j * chunk : (j + 1) * chunk] = shift.T
        flow_ref[j * chunk : (j + 1) * chunk] = flows[j][...].T


def shift_flows(step, flows, ends, factors):
    n = len(flows)
    lines, chunk = flows[0].shape
    out = jax.ShapeDtypeStruct((n * chunk, lines), F32)
    return pl.pallas_call(
        functools.partial(shift_kernel, n),
        out_shape=[out, out],
        compiler_params=kernel_params(16),
        cost_estimate=cost(3e9, 4 * n * chunk * lines * 4),
        name="shift",
    )(step, *flows, *ends, *factors)


def finish_kernel(entries, tally_ref, step_ref, policy_ref, flow_ref, shift_ref, *outs):
    policy_out, flow_out, decrement_out, norm_out = outs
    feats = policy_ref.shape[0]
    groups = tally_ref.shape[0] // 8
    total = tally_ref[0:1]
    for j in range(1, groups):
        total = total + tally_ref[8 * j : 8 * j + 1]
    root = jnp.sqrt(total)
    length = 1.0 / (1.0 + jnp.sqrt(total[:, feats : feats + 1] / (barrier_weight * entries)))
    policy_out[...] = policy_ref[...] + length * step_ref[...].T[0:feats]
    flow_out[...] = flow_ref[...] + length * shift_ref[...]
    decrement_out[...] = root[:, feats : feats + 1]
    norm_out[...] = root[:, feats + 1 : feats + 2]


def finish(entries, tallies, step, policy, flow, shift):
    one = jax.ShapeDtypeStruct((1, 1), F32)
    return pl.pallas_call(
        functools.partial(finish_kernel, entries),
        out_shape=[
            jax.ShapeDtypeStruct(policy.shape, F32),
            jax.ShapeDtypeStruct(flow.shape, F32),
            one,
            one,
        ],
        compiler_params=kernel_params(16),
        cost_estimate=cost(1e9, 12 * flow.size),
        name="finish",
    )(tallies, step, policy, flow, shift)


def swap(a, axis):
    return lax.ppermute(a, axis, [(0, 1), (1, 0)])


def shards(
    wind_dev, ptdf, region_weights, incidence, monitored, ratings, base_flow, line_cost, policy
):
    zs, ys = lax.axis_size("line_0"), lax.axis_size("line_1")
    z, y, core = lax.axis_index("line_0"), lax.axis_index("line_1"), lax.axis_index("sample_2")
    assert ys == 2 and zs % 2 == 0
    scen_here, width = wind_dev.shape
    lines_here = ptdf.shape[0]
    features = policy.shape[0]
    padded = -(-width // 128) * 128
    groups = scen_here // CHUNK
    up_ring = [(i, (i + 1) % zs) for i in range(zs)]
    down_ring = [(i, (i - 1) % zs) for i in range(zs)]

    wind = wind_dev.T
    chunks = [wind[:, j * CHUNK : (j + 1) * CHUNK] for j in range(groups)]
    half = lines_here // 2
    outgoing = repack(ptdf.T, True, 1 - y, core, half, zs, width, padded)
    part_a = swap(outgoing, "line_1")
    part_b = swap(part_a, "sample_2")
    endpoints = jnp.stack(
        [jnp.take(incidence[:, 0], monitored), jnp.take(incidence[:, 1], monitored)], axis=1
    )
    rating = jnp.take(ratings, monitored)

    gathered = []
    for j, own in enumerate(chunks):
        if j >= AHEAD:
            own, gathered[j - AHEAD] = lax.optimization_barrier((own, gathered[j - AHEAD]))
        pieces, up, down = [own], own, own
        for t in range(1, zs // 2):
            up = lax.ppermute(up, "line_0", up_ring)
            down = lax.ppermute(down, "line_0", down_ring)
            pieces += [up, down]
        if j % 2 == 0:
            pieces.append(lax.ppermute(up, "line_0", up_ring))
        else:
            pieces.append(lax.ppermute(down, "line_0", down_ring))
        gathered.append(pieces)

    own_ptdf = repack(ptdf.T, True, y, 0, lines_here, zs, width, padded)
    regions = jnp.pad(region_weights, ((0, features - region_weights.shape[0]), (0, 0)))
    region = repack(regions, False, y, 0, features, zs, width, padded)
    ends = ends_blocks(endpoints, y, zs, width, padded)
    part_ends = ends_blocks(swap(endpoints, "line_1"), y, zs, width, padded)
    rhs = (own_ptdf, ends, region, part_a, part_b, part_ends)

    order = [0]
    for t in range(1, zs // 2):
        order += [-t, t]
    order.append(zs // 2)
    meta = jnp.stack([(z + t) % zs for t in order] + [core]).astype(jnp.int32)
    per_line = jnp.stack([base_flow, rating], axis=1)
    policy_t = policy.T
    flows, all_ends, factors, sums = [], [], [], None
    for pieces in gathered:
        own, send = partial_flows(meta, pieces, rhs, padded)
        got = swap(send, "line_1")
        flow, end, factor, sums = penalty(own, got, per_line, policy_t, sums)
        flows.append(flow)
        all_ends.append(end)
        factors.append(factor)

    copies = lax.axis_size(SAMPLE)
    share = lines_here // copies
    sums = lax.all_to_all(sums, SAMPLE, split_axis=0, concat_axis=0, tiled=True)
    at = lax.axis_index(SAMPLE) * share
    policy_part = jnp.pad(
        lax.dynamic_slice_in_dim(policy, at, share, 1), ((0, 0), (0, 128 - share))
    )
    weight = lax.dynamic_slice_in_dim(line_cost, at, share, 0) / (scen_here * copies)
    weight = jnp.broadcast_to(jnp.pad(weight, (0, 128 - share))[None, :], (8, 128))
    step = solve(sums, weight, policy_part, copies)
    step = lax.all_to_all(step, SAMPLE, split_axis=0, concat_axis=0, tiled=True)
    lines_axis = lax.axis_size(LINE)
    tallies = lax.all_to_all(
        tally(step, lines_axis), LINE, split_axis=0, concat_axis=0, tiled=True
    )
    flow, shift = shift_flows(step, flows, all_ends, factors)
    entries = features * lines_here * lines_axis
    new_policy, new_flows, decrement, norm = finish(entries, tallies, step, policy, flow, shift)
    return (new_policy, new_flows, decrement[0, 0], norm[0, 0])


def solution(mesh):
    torus = Mesh(
        mesh.devices.reshape(2, 4, 2, 8, 2),
        ("sample_0", "sample_1", "sample_2", "line_0", "line_1"),
    )
    return jax.shard_map(
        shards,
        mesh=torus,
        in_specs=(
            P(SAMPLE, LINE),
            P(LINE, None),
            P(),
            P(),
            P(LINE),
            P(),
            P(LINE),
            P(LINE),
            P(None, LINE),
        ),
        out_specs=(P(None, LINE), P(SAMPLE, LINE), P(), P()),
        check_vma=False,
    )
```

```python
import functools

import jax
import jax.numpy as jnp
from jax import lax
from jax.experimental import pallas as pl
from jax.experimental.pallas import tpu as pltpu
from jax.sharding import Mesh
from jax.sharding import PartitionSpec as P


LINE = ("line_0", "line_1")
SAMPLE = ("sample_0", "sample_1", "sample_2")


ridge_weight = 1.0
barrier_weight = 0.1
smoothing = 0.5

HIGHEST = lax.Precision.HIGHEST
F32 = jnp.float32
BF16 = jnp.bfloat16
NT = (((1,), (1,)), ((), ()))
CHUNK = 256
MIB = 1 << 20


def row_blocks(a):
    return a // 8 + 1


def row_starts(features):
    starts, at = [], 0
    for a in range(features):
        starts.append(at)
        at += 8 * row_blocks(a)
    return starts, at


def kernel_params(vmem_mib):
    return pltpu.CompilerParams(vmem_limit_bytes=vmem_mib * MIB)


def cost(flops, nbytes):
    return pl.CostEstimate(flops=int(flops), bytes_accessed=int(nbytes), transcendentals=0)


def repack_kernel(width, padded, turned, meta, rows_ref, out_ref):
    lines, total = out_ref.shape
    for parity in (0, 1):

        @pl.when(meta[0] == parity)
        def _():
            for b in range(total // padded):
                start, at = width * (2 * b + parity), b * padded
                tail = at + width // 128 * 128
                out_ref[:, tail : at + padded] = jnp.zeros(
                    (lines, at + padded - tail), out_ref.dtype
                )
                if turned:
                    low = start // 16 * 16
                    first = pl.multiple_of(meta[1] * lines, lines)
                    window = rows_ref[low : low + padded, pl.ds(first, lines)].T
                    out_ref[:, at : at + width] = window[:, start - low : start - low + width]
                else:
                    out_ref[:, at : at + width] = rows_ref[:, start : start + width]


def repack(rows, turned, parity, first, lines, blocks, width, padded):
    meta = jnp.stack([parity, jnp.int32(first)]).astype(jnp.int32)
    if turned:
        assert all(width * b % 16 + width <= padded for b in range(2 * blocks))
        assert all(width * b // 16 * 16 + padded <= rows.shape[0] for b in range(2 * blocks))
    return pl.pallas_call(
        functools.partial(repack_kernel, width, padded, turned),
        grid_spec=pltpu.PrefetchScalarGridSpec(
            num_scalar_prefetch=1,
            in_specs=[pl.BlockSpec(memory_space=pltpu.VMEM)],
            out_specs=pl.BlockSpec(memory_space=pltpu.VMEM),
        ),
        out_shape=jax.ShapeDtypeStruct((lines, blocks * padded), rows.dtype),
        compiler_params=kernel_params(24),
        cost_estimate=cost(3e9, 2 * rows.size),
        name="repack",
    )(meta, rows)


def ends_kernel(width, padded, meta, ids_ref, out_ref):
    lines, total = out_ref.shape
    lane = lax.broadcasted_iota(jnp.int32, (lines, padded), 1)
    lane = jnp.where(lane < width, lane, -1)
    for b in range(total // padded):
        base = width * (2 * b + meta[0])
        first, last = ids_ref[:, 0:1] - base, ids_ref[:, 1:2] - base
        first = jnp.where(first < 0, -2, first)
        last = jnp.where(last < 0, -2, last)
        hits = jnp.where(lane == last, 1.0, 0.0) - jnp.where(lane == first, 1.0, 0.0)
        out_ref[:, b * padded : (b + 1) * padded] = hits.astype(out_ref.dtype)


def ends_blocks(ids, parity, blocks, width, padded):
    lines = ids.shape[0]
    return pl.pallas_call(
        functools.partial(ends_kernel, width, padded),
        grid_spec=pltpu.PrefetchScalarGridSpec(
            num_scalar_prefetch=1,
            in_specs=[pl.BlockSpec(memory_space=pltpu.VMEM)],
            out_specs=pl.BlockSpec(memory_space=pltpu.VMEM),
        ),
        out_shape=jax.ShapeDtypeStruct((lines, blocks * padded), BF16),
        compiler_params=kernel_params(16),
        cost_estimate=cost(3e9, 2 * blocks * lines * padded),
        name="ends",
    )(jnp.stack([parity]).astype(jnp.int32), ids)


def place(held, at, piece, padded):
    width = piece.shape[0]
    even = width // 16 * 16
    held[pl.ds(at + even, padded - even)] = jnp.zeros((padded - even, held.shape[1]), held.dtype)
    held[pl.ds(at, even)] = piece[0:even]
    held[pl.ds(at + even, width - even)] = piece[even:width]


def flows_kernel(n, padded, last, meta, *refs):
    pieces, rhs, refs = refs[:n], refs[n : n + 6], refs[n + 6 :]
    own_ref, send_ref, held = refs[-3:]
    ptdf_ref, ends_ref, region_ref, part_a_ref, part_b_ref, part_ends_ref = rhs
    lines = ptdf_ref.shape[0]
    rest = pl.multiple_of(meta[BLOCKS - 1] * padded, padded)
    if last:
        place(held, 0, pieces[0], padded)
    else:
        for j in range(n):
            place(held, pl.multiple_of(meta[j] * padded, padded), pieces[j], padded)
        held[pl.ds(rest, padded)] = jnp.zeros((padded, held.shape[1]), held.dtype)

    def add(old_ref, new_ref, rows, x):
        left = x[:, pl.ds(rest, padded)] if last else x[...]
        out = jnp.dot(left, held[...], preferred_element_type=F32)
        new_ref[rows] = old_ref[rows] + out if last else out

    old_own, old_send = refs[0:2] if last else (None, None)
    half = lines // 2
    first = pl.multiple_of(meta[BLOCKS] * half, half)
    second = pl.multiple_of((1 - meta[BLOCKS]) * half, half)
    add(old_send, send_ref, pl.ds(first, half), part_a_ref)
    add(old_send, send_ref, pl.ds(second, half), part_b_ref)
    add(old_send, send_ref, pl.ds(lines, lines), part_ends_ref)
    factor_rows = pl.ds(2 * lines, region_ref.shape[0])
    add(old_send, send_ref, factor_rows, region_ref)
    own_ref[factor_rows] = send_ref[factor_rows]
    add(old_own, own_ref, pl.ds(0, lines), ptdf_ref)
    add(old_own, own_ref, pl.ds(lines, lines), ends_ref)


BLOCKS = 8


def partial_flows(meta, pieces, rhs, padded, old):
    n = len(pieces)
    chunk = pieces[0].shape[1]
    total = 2 * rhs[0].shape[0] + rhs[2].shape[0]
    whole = pl.BlockSpec(memory_space=pltpu.VMEM)
    out = jax.ShapeDtypeStruct((total, chunk), F32)
    last = old is not None
    args = list(pieces) + list(rhs) + (list(old) if last else [])
    return pl.pallas_call(
        functools.partial(flows_kernel, n, padded, last),
        grid_spec=pltpu.PrefetchScalarGridSpec(
            num_scalar_prefetch=1,
            in_specs=[whole] * len(args),
            out_specs=[whole, whole],
            scratch_shapes=[pltpu.VMEM((padded if last else BLOCKS * padded, chunk), BF16)],
        ),
        out_shape=[out, out],
        compiler_params=kernel_params(20),
        cost_estimate=cost(6e9, n * 4 * padded * total),
        name="flows",
    )(meta, *args)


def sigmoid(x):
    return 1.0 / (1.0 + jnp.exp(-x))


def parts_of(x):
    high = x.astype(BF16)
    return high, (x - high.astype(F32)).astype(BF16)


def times_rows(left, rows):
    right = jnp.concatenate(rows, axis=0)
    (lh, ll), (rh, rl) = parts_of(left), parts_of(right)

    def dot(a, b):
        return lax.dot_general(a, b, NT, preferred_element_type=F32)

    return dot(lh, rh) + (dot(lh, rl) + dot(ll, rh))


def penalty_kernel(has_prev, own_ref, got_ref, line_ref, policy_ref, *refs):
    prev_ref = refs[0] if has_prev else None
    flow_ref, ends_ref, factor_ref, sums_ref = refs[1 if has_prev else 0 :]
    lines = flow_ref.shape[0]
    feats, chunk = factor_ref.shape
    both = own_ref[...] + got_ref[...]
    grid_flow, ends, factors = both[0:lines], both[lines : 2 * lines], both[2 * lines :]
    policy = policy_ref[...]
    flow = (
        grid_flow
        + line_ref[:, 0:1]
        + jnp.dot(policy, factors, precision=HIGHEST, preferred_element_type=F32)
        + policy[:, feats - 1 : feats] * ends
    )
    rating = line_ref[:, 1:2]
    up = sigmoid((flow - rating) / smoothing)
    down = sigmoid((-flow - rating) / smoothing)
    slope = up - down
    curve = (up * (1.0 - up) + down * (1.0 - down)) / smoothing
    weighted = curve * ends
    sub = lax.broadcasted_iota(jnp.int32, (8, chunk), 0)
    zero = jnp.zeros((8, chunk), F32)
    products, lifted, sloped = [], [], []
    for a in range(feats):
        g = a // 8
        group = factors[8 * g : 8 * g + 8]
        keep = group * factors[a : a + 1] if a < feats - 1 else zero
        slot = None
        if a % 8 == 0:
            keep, slot = jnp.where(sub == 0, keep, 0.0), jnp.where(sub > 0, group, 0.0)
        elif a % 8 == 1:
            keep = jnp.where(sub < 7, keep, 0.0)
            slot = jnp.where(sub == 7, factors[8 * g : 8 * g + 1], 0.0)
        for h in range(g):
            rows = factors[8 * h : 8 * h + 8]
            products.append(rows * factors[a : a + 1] if a < feats - 1 else zero)
            lifted.append(rows if a == feats - 1 else None)
            sloped.append(None)
        products.append(keep)
        lifted.append(group if a == feats - 1 else None)
        sloped.append(slot)
    tiles = []
    for at in range(0, len(products), 16):
        tile = times_rows(curve, products[at : at + 16])
        for left, rows in ((weighted, lifted[at : at + 16]), (slope, sloped[at : at + 16])):
            if any(r is not None for r in rows):
                tile = tile + times_rows(left, [zero if r is None else r for r in rows])
        tiles.append(tile)
    sums = jnp.concatenate(tiles, axis=1)
    starts, size = row_starts(feats)
    corner = jnp.sum(weighted * ends, axis=1, keepdims=True)
    last = jnp.sum(slope * ends, axis=1, keepdims=True)
    last_at = starts[feats - 8] + feats - 1
    col = lax.broadcasted_iota(jnp.int32, (lines, size), 1)
    sums = sums + jnp.where(col == size - 1, corner, 0.0) + jnp.where(col == last_at, last, 0.0)
    if has_prev:
        sums = sums + prev_ref[...]
    sums_ref[...] = sums
    flow_ref[...] = flow
    ends_ref[...] = ends
    factor_ref[...] = factors


def penalty(own, got, per_line, policy_t, prev):
    lines, feats = policy_t.shape
    chunk = own.shape[1]
    size = row_starts(feats)[1]
    args = [own, got, per_line, policy_t] + ([] if prev is None else [prev])
    return pl.pallas_call(
        functools.partial(penalty_kernel, prev is not None),
        out_shape=[
            jax.ShapeDtypeStruct((lines, chunk), F32),
            jax.ShapeDtypeStruct((lines, chunk), F32),
            jax.ShapeDtypeStruct((feats, chunk), F32),
            jax.ShapeDtypeStruct((lines, size), F32),
        ],
        compiler_params=kernel_params(24),
        cost_estimate=cost(3e9, 4 * lines * (size * 2 + chunk * 6)),
        name="penalty",
    )(*args)


def solve_kernel(copies, lines, sums_ref, weight_ref, policy_ref, out_ref, rows_ref):
    feats = policy_ref.shape[0]
    starts, _ = row_starts(feats)
    total = sums_ref[0:lines]
    for src in range(1, copies):
        total = total + sums_ref[src * lines : (src + 1) * lines]
    square = jnp.concatenate([total, jnp.zeros((128 - lines, total.shape[1]), F32)], axis=0)
    weight = weight_ref[0:1]
    policy = policy_ref[...]
    margin = 1.0 - policy * policy
    diag = ridge_weight + barrier_weight * 2.0 * (1.0 + policy * policy) / (margin * margin)
    rows_ref[...] = square.T * weight
    sub = lax.broadcasted_iota(jnp.int32, (8, 128), 0)
    parts = []
    for q in range(feats // 8):
        top, next_row = starts[8 * q] + 8 * q, starts[8 * q + 1] + 8 * q
        parts.append(
            jnp.where(
                sub == 0, rows_ref[next_row + 7 : next_row + 8], rows_ref[top : top + 8]
            )
        )
    g = (
        jnp.concatenate(parts, axis=0)
        + ridge_weight * policy
        + barrier_weight * 2.0 * policy / margin
    )
    norm = jnp.sum(g * g, axis=0, keepdims=True)
    row = lax.broadcasted_iota(jnp.int32, (feats, 128), 0)
    for a in range(feats):
        at = starts[a] + 8 * (a // 8)
        rows_ref[at : at + 8] += jnp.where(sub == a % 8, diag[a : a + 1], 0.0)
    decrement = jnp.zeros((1, 128), F32)
    inverses = [None] * feats
    for c in reversed(range(feats)):
        height = 8 * row_blocks(c)
        pivot = rows_ref[starts[c] : starts[c] + height]
        inverse = 1.0 / pivot[c : c + 1]
        inverses[c] = inverse
        g_c = g[c : c + 1]
        decrement = decrement + g_c * g_c * inverse
        scaled = pivot * inverse
        for i in range(c):
            tall = 8 * row_blocks(i)
            rows_ref[starts[i] : starts[i] + tall] -= scaled[i : i + 1] * pivot[0:tall]
        full = scaled
        if height < feats:
            full = jnp.concatenate([scaled, jnp.zeros((feats - height, 128), F32)], axis=0)
        g = g - jnp.where(row < c, full * g_c, 0.0)
    x = jnp.zeros((feats, 128), F32)
    for i in range(feats):
        height = 8 * row_blocks(i)
        known = jnp.sum(
            rows_ref[starts[i] : starts[i] + height] * x[0:height], axis=0, keepdims=True
        )
        x_i = (g[i : i + 1] - known) * inverses[i]
        x = jnp.where(row == i, x_i, x)
    tail = jnp.concatenate([decrement, norm, jnp.zeros((128 - feats - 2, 128), F32)], axis=0)
    result = jnp.concatenate([-x, tail], axis=0).T[0:lines]
    for dst in range(copies):
        out_ref[dst * lines : (dst + 1) * lines] = result


def solve(sums, weight, policy_part, copies):
    lines = sums.shape[0] // copies
    return pl.pallas_call(
        functools.partial(solve_kernel, copies, lines),
        out_shape=jax.ShapeDtypeStruct((copies * lines, 128), F32),
        scratch_shapes=[pltpu.VMEM((sums.shape[1], 128), F32)],
        compiler_params=kernel_params(16),
        cost_estimate=cost(1e9, 4 * sums.size),
        name="solve",
    )(sums, weight, policy_part)


def tally_kernel(step_ref, out_ref):
    out_ref[...] = jnp.broadcast_to(jnp.sum(step_ref[...], axis=0, keepdims=True), out_ref.shape)


def tally(step, groups):
    return pl.pallas_call(
        tally_kernel,
        out_shape=jax.ShapeDtypeStruct((8 * groups, 128), F32),
        compiler_params=kernel_params(8),
        name="tally",
    )(step)


def shift_kernel(n, step_ref, *refs):
    flows, ends, factors = refs[:n], refs[n : 2 * n], refs[2 * n : 3 * n]
    flow_ref, shift_ref = refs[3 * n :]
    feats, chunk = factors[0].shape
    step = step_ref[...]
    for j in range(n):
        shift = (
            jnp.dot(step[:, 0:feats], factors[j][...], precision=HIGHEST, preferred_element_type=F32)
            + step[:, feats - 1 : feats] * ends[j][...]
        )
        shift_ref[j * chunk : (j + 1) * chunk] = shift.T
        flow_ref[j * chunk : (j + 1) * chunk] = flows[j][...].T


def shift_flows(step, flows, ends, factors):
    n = len(flows)
    lines, chunk = flows[0].shape
    out = jax.ShapeDtypeStruct((n * chunk, lines), F32)
    return pl.pallas_call(
        functools.partial(shift_kernel, n),
        out_shape=[out, out],
        compiler_params=kernel_params(16),
        cost_estimate=cost(3e9, 4 * n * chunk * lines * 4),
        name="shift",
    )(step, *flows, *ends, *factors)


def finish_kernel(entries, tally_ref, step_ref, policy_ref, flow_ref, shift_ref, *outs):
    policy_out, flow_out, decrement_out, norm_out = outs
    feats = policy_ref.shape[0]
    groups = tally_ref.shape[0] // 8
    total = tally_ref[0:1]
    for j in range(1, groups):
        total = total + tally_ref[8 * j : 8 * j + 1]
    root = jnp.sqrt(total)
    length = 1.0 / (1.0 + jnp.sqrt(total[:, feats : feats + 1] / (barrier_weight * entries)))
    policy_out[...] = policy_ref[...] + length * step_ref[...].T[0:feats]
    flow_out[...] = flow_ref[...] + length * shift_ref[...]
    decrement_out[...] = root[:, feats : feats + 1]
    norm_out[...] = root[:, feats + 1 : feats + 2]


def finish(entries, tallies, step, policy, flow, shift):
    one = jax.ShapeDtypeStruct((1, 1), F32)
    return pl.pallas_call(
        functools.partial(finish_kernel, entries),
        out_shape=[
            jax.ShapeDtypeStruct(policy.shape, F32),
            jax.ShapeDtypeStruct(flow.shape, F32),
            one,
            one,
        ],
        compiler_params=kernel_params(16),
        cost_estimate=cost(1e9, 12 * flow.size),
        name="finish",
    )(tallies, step, policy, flow, shift)


def swap(a, axis):
    return lax.ppermute(a, axis, [(0, 1), (1, 0)])


def step_on_shards(
    wind_dev, ptdf, region_weights, incidence, monitored, ratings, base_flow, line_cost, policy
):
    zs, ys = lax.axis_size("line_0"), lax.axis_size("line_1")
    z, y, core = lax.axis_index("line_0"), lax.axis_index("line_1"), lax.axis_index("sample_2")
    assert ys == 2 and zs % 2 == 0
    scen_here, width = wind_dev.shape
    lines_here = ptdf.shape[0]
    features = policy.shape[0]
    padded = -(-width // 128) * 128
    groups = scen_here // CHUNK
    up_ring = [(i, (i + 1) % zs) for i in range(zs)]
    down_ring = [(i, (i - 1) % zs) for i in range(zs)]

    wind = wind_dev.T
    chunks = [wind[:, j * CHUNK : (j + 1) * CHUNK] for j in range(groups)]
    half = lines_here // 2
    outgoing = repack(ptdf.T, True, 1 - y, core, half, zs, width, padded)
    part_a = swap(outgoing, "line_1")
    part_b = swap(part_a, "sample_2")
    endpoints = jnp.stack(
        [jnp.take(incidence[:, 0], monitored), jnp.take(incidence[:, 1], monitored)], axis=1
    )
    rating = jnp.take(ratings, monitored)

    assert zs == BLOCKS
    gathered = []
    for j, own in enumerate(chunks):
        pieces, up, down = [own], own, own
        for _ in range(1, zs // 2):
            up = lax.ppermute(up, "line_0", up_ring)
            down = lax.ppermute(down, "line_0", down_ring)
            pieces += [up, down]
        if j % 2 == 0:
            pieces.append(lax.ppermute(up, "line_0", up_ring))
        else:
            pieces.append(lax.ppermute(down, "line_0", down_ring))
        gathered.append(pieces)

    own_ptdf = repack(ptdf.T, True, y, 0, lines_here, zs, width, padded)
    regions = jnp.pad(region_weights, ((0, features - region_weights.shape[0]), (0, 0)))
    region = repack(regions, False, y, 0, features, zs, width, padded)
    ends = ends_blocks(endpoints, y, zs, width, padded)
    part_points = swap(endpoints, "line_1")
    part_ends = ends_blocks(part_points, y, zs, width, padded)
    rhs = (own_ptdf, ends, region, part_a, part_b, part_ends)

    order = [0]
    for t in range(1, zs // 2):
        order += [-t, t]
    order.append(zs // 2)
    meta = jnp.stack([(z + t) % zs for t in order] + [core]).astype(jnp.int32)
    per_line = jnp.stack([base_flow, rating], axis=1)
    policy_t = policy.T
    flows, all_ends, factors, sums = [], [], [], None
    for pieces in gathered:
        early = partial_flows(meta, pieces[:-1], rhs, padded, None)
        own, send = partial_flows(meta, pieces[-1:], rhs, padded, early)
        got = swap(send, "line_1")
        flow, end, factor, sums = penalty(own, got, per_line, policy_t, sums)
        flows.append(flow)
        all_ends.append(end)
        factors.append(factor)

    copies = lax.axis_size(SAMPLE)
    share = lines_here // copies
    sums = lax.all_to_all(sums, SAMPLE, split_axis=0, concat_axis=0, tiled=True)
    at = lax.axis_index(SAMPLE) * share
    policy_part = jnp.pad(
        lax.dynamic_slice_in_dim(policy, at, share, 1), ((0, 0), (0, 128 - share))
    )
    weight = lax.dynamic_slice_in_dim(line_cost, at, share, 0) / (scen_here * copies)
    weight = jnp.broadcast_to(jnp.pad(weight, (0, 128 - share))[None, :], (8, 128))
    step = solve(sums, weight, policy_part, copies)
    step = lax.all_to_all(step, SAMPLE, split_axis=0, concat_axis=0, tiled=True)
    lines_axis = lax.axis_size(LINE)
    tallies = lax.all_to_all(
        tally(step, lines_axis), LINE, split_axis=0, concat_axis=0, tiled=True
    )
    flow, shift = shift_flows(step, flows, all_ends, factors)
    entries = features * lines_here * lines_axis
    new_policy, new_flows, decrement, norm = finish(entries, tallies, step, policy, flow, shift)
    return (new_policy, new_flows, decrement[0, 0], norm[0, 0])


def solution(mesh):
    torus = Mesh(
        mesh.devices.reshape(2, 4, 2, 8, 2),
        ("sample_0", "sample_1", "sample_2", "line_0", "line_1"),
    )
    return jax.shard_map(
        step_on_shards,
        mesh=torus,
        in_specs=(
            P(SAMPLE, LINE),
            P(LINE, None),
            P(),
            P(),
            P(LINE),
            P(),
            P(LINE),
            P(LINE),
            P(None, LINE),
        ),
        out_specs=(P(None, LINE), P(SAMPLE, LINE), P(), P()),
        check_vma=False,
    )
```

```python
import functools

import jax
import jax.numpy as jnp
from jax import lax
from jax.experimental import pallas as pl
from jax.experimental.pallas import tpu as pltpu
from jax.sharding import Mesh
from jax.sharding import PartitionSpec as P


LINE = ("line_0", "line_1")
SAMPLE = ("sample_0", "sample_1", "sample_2")


ridge_weight = 1.0
barrier_weight = 0.1
smoothing = 0.5

HIGHEST = lax.Precision.HIGHEST
F32 = jnp.float32
BF16 = jnp.bfloat16
NT = (((1,), (1,)), ((), ()))
CHUNK = 256
MIB = 1 << 20


def row_blocks(a):
    return a // 8 + 1


def row_starts(features):
    starts, at = [], 0
    for a in range(features):
        starts.append(at)
        at += 8 * row_blocks(a)
    return starts, at


def kernel_params(vmem_mib):
    return pltpu.CompilerParams(vmem_limit_bytes=vmem_mib * MIB)


def cost(flops, nbytes):
    return pl.CostEstimate(flops=int(flops), bytes_accessed=int(nbytes), transcendentals=0)


def repack_kernel(width, padded, turned, meta, rows_ref, out_ref):
    lines, total = out_ref.shape
    for parity in (0, 1):

        @pl.when(meta[0] == parity)
        def _():
            for b in range(total // padded):
                start, at = width * (2 * b + parity), b * padded
                tail = at + width // 128 * 128
                out_ref[:, tail : at + padded] = jnp.zeros(
                    (lines, at + padded - tail), out_ref.dtype
                )
                if turned:
                    low = start // 16 * 16
                    first = pl.multiple_of(meta[1] * lines, lines)
                    window = rows_ref[low : low + padded, pl.ds(first, lines)].T
                    out_ref[:, at : at + width] = window[:, start - low : start - low + width]
                else:
                    count = rows_ref.shape[0]
                    if count < lines:
                        out_ref[:, at : at + padded] = jnp.zeros((lines, padded), out_ref.dtype)
                    out_ref[0:count, at : at + width] = rows_ref[:, start : start + width]


def repack(rows, turned, parity, first, lines, blocks, width, padded):
    meta = jnp.stack([parity, jnp.int32(first)]).astype(jnp.int32)
    if turned:
        assert all(width * b % 16 + width <= padded for b in range(2 * blocks))
        assert all(width * b // 16 * 16 + padded <= rows.shape[0] for b in range(2 * blocks))
    return pl.pallas_call(
        functools.partial(repack_kernel, width, padded, turned),
        grid_spec=pltpu.PrefetchScalarGridSpec(
            num_scalar_prefetch=1,
            in_specs=[pl.BlockSpec(memory_space=pltpu.VMEM)],
            out_specs=pl.BlockSpec(memory_space=pltpu.VMEM),
        ),
        out_shape=jax.ShapeDtypeStruct((lines, blocks * padded), rows.dtype),
        compiler_params=kernel_params(24),
        cost_estimate=cost(3e9, 2 * rows.size),
        name="repack",
    )(meta, rows)


def ends_kernel(width, padded, meta, ids_ref, out_ref):
    lines, total = out_ref.shape
    lane = lax.broadcasted_iota(jnp.int32, (lines, padded), 1)
    lane = jnp.where(lane < width, lane, -1)
    for b in range(total // padded):
        base = width * (2 * b + meta[0])
        first, last = ids_ref[:, 0:1] - base, ids_ref[:, 1:2] - base
        first = jnp.where(first < 0, -2, first)
        last = jnp.where(last < 0, -2, last)
        hits = jnp.where(lane == last, 1.0, 0.0) - jnp.where(lane == first, 1.0, 0.0)
        out_ref[:, b * padded : (b + 1) * padded] = hits.astype(out_ref.dtype)


def ends_blocks(ids, parity, blocks, width, padded):
    lines = ids.shape[0]
    return pl.pallas_call(
        functools.partial(ends_kernel, width, padded),
        grid_spec=pltpu.PrefetchScalarGridSpec(
            num_scalar_prefetch=1,
            in_specs=[pl.BlockSpec(memory_space=pltpu.VMEM)],
            out_specs=pl.BlockSpec(memory_space=pltpu.VMEM),
        ),
        out_shape=jax.ShapeDtypeStruct((lines, blocks * padded), BF16),
        compiler_params=kernel_params(16),
        cost_estimate=cost(3e9, 2 * blocks * lines * padded),
        name="ends",
    )(jnp.stack([parity]).astype(jnp.int32), ids)


def place(held, at, piece, padded):
    width = piece.shape[0]
    even = width // 16 * 16
    held[pl.ds(at + even, padded - even)] = jnp.zeros((padded - even, held.shape[1]), held.dtype)
    held[pl.ds(at, even)] = piece[0:even]
    held[pl.ds(at + even, width - even)] = piece[even:width]


def flows_kernel(n, padded, last, meta, *refs):
    pieces, rhs, refs = refs[:n], refs[n : n + 6], refs[n + 6 :]
    own_ref, send_ref, held = refs[-3:]
    ptdf_ref, ends_ref, region_ref, part_a_ref, part_b_ref, part_ends_ref = rhs
    lines = ptdf_ref.shape[0]
    rest = pl.multiple_of(meta[BLOCKS - 1] * padded, padded)
    if last:
        place(held, 0, pieces[0], padded)
    else:
        for j in range(n):
            place(held, pl.multiple_of(meta[j] * padded, padded), pieces[j], padded)
        held[pl.ds(rest, padded)] = jnp.zeros((padded, held.shape[1]), held.dtype)

    def add(old_ref, new_ref, rows, x):
        left = x[:, pl.ds(rest, padded)] if last else x[...]
        out = jnp.dot(left, held[...], preferred_element_type=F32)
        new_ref[rows] = old_ref[rows] + out if last else out

    old_own, old_send = refs[0:2] if last else (None, None)
    half = lines // 2
    first = pl.multiple_of(meta[BLOCKS] * half, half)
    second = pl.multiple_of((1 - meta[BLOCKS]) * half, half)
    add(old_send, send_ref, pl.ds(first, half), part_a_ref)
    add(old_send, send_ref, pl.ds(second, half), part_b_ref)
    add(old_send, send_ref, pl.ds(lines, lines), part_ends_ref)
    factor_rows = pl.ds(2 * lines, region_ref.shape[0])
    add(old_send, send_ref, factor_rows, region_ref)
    own_ref[factor_rows] = send_ref[factor_rows]
    add(old_own, own_ref, pl.ds(0, lines), ptdf_ref)
    add(old_own, own_ref, pl.ds(lines, lines), ends_ref)


BLOCKS = 8


def partial_flows(meta, pieces, rhs, padded, old):
    n = len(pieces)
    chunk = pieces[0].shape[1]
    total = 2 * rhs[0].shape[0] + rhs[2].shape[0]
    whole = pl.BlockSpec(memory_space=pltpu.VMEM)
    out = jax.ShapeDtypeStruct((total, chunk), F32)
    last = old is not None
    args = list(pieces) + list(rhs) + (list(old) if last else [])
    return pl.pallas_call(
        functools.partial(flows_kernel, n, padded, last),
        grid_spec=pltpu.PrefetchScalarGridSpec(
            num_scalar_prefetch=1,
            in_specs=[whole] * len(args),
            out_specs=[whole, whole],
            scratch_shapes=[pltpu.VMEM((padded if last else BLOCKS * padded, chunk), BF16)],
        ),
        out_shape=[out, out],
        compiler_params=kernel_params(20),
        cost_estimate=cost(6e9, n * 4 * padded * total),
        name="flows",
    )(meta, *args)


def sigmoid(x):
    return 1.0 / (1.0 + jnp.exp(-x))


def parts_of(x):
    high = x.astype(BF16)
    return high, (x - high.astype(F32)).astype(BF16)


def times_rows(left, rows):
    right = jnp.concatenate(rows, axis=0)
    (lh, ll), (rh, rl) = parts_of(left), parts_of(right)

    def dot(a, b):
        return lax.dot_general(a, b, NT, preferred_element_type=F32)

    return dot(lh, rh) + (dot(lh, rl) + dot(ll, rh))


def penalty_kernel(has_prev, own_ref, got_ref, line_ref, policy_ref, *refs):
    prev_ref = refs[0] if has_prev else None
    flow_ref, ends_ref, factor_ref, sums_ref = refs[1 if has_prev else 0 :]
    lines = flow_ref.shape[0]
    feats, chunk = factor_ref.shape
    both = own_ref[...] + got_ref[...]
    grid_flow, ends, factors = both[0:lines], both[lines : 2 * lines], both[2 * lines :]
    policy = policy_ref[...]
    flow = (
        grid_flow
        + line_ref[:, 0:1]
        + jnp.dot(policy, factors, precision=HIGHEST, preferred_element_type=F32)
        + policy[:, feats - 1 : feats] * ends
    )
    rating = line_ref[:, 1:2]
    up = sigmoid((flow - rating) / smoothing)
    down = sigmoid((-flow - rating) / smoothing)
    slope = up - down
    curve = (up * (1.0 - up) + down * (1.0 - down)) / smoothing
    weighted = curve * ends
    sub = lax.broadcasted_iota(jnp.int32, (8, chunk), 0)
    zero = jnp.zeros((8, chunk), F32)
    products, lifted, sloped = [], [], []
    for a in range(feats):
        g = a // 8
        group = factors[8 * g : 8 * g + 8]
        keep = group * factors[a : a + 1] if a < feats - 1 else zero
        slot = None
        if a % 8 == 0:
            keep, slot = jnp.where(sub == 0, keep, 0.0), jnp.where(sub > 0, group, 0.0)
        elif a % 8 == 1:
            keep = jnp.where(sub < 7, keep, 0.0)
            slot = jnp.where(sub == 7, factors[8 * g : 8 * g + 1], 0.0)
        for h in range(g):
            rows = factors[8 * h : 8 * h + 8]
            products.append(rows * factors[a : a + 1] if a < feats - 1 else zero)
            lifted.append(rows if a == feats - 1 else None)
            sloped.append(None)
        products.append(keep)
        lifted.append(group if a == feats - 1 else None)
        sloped.append(slot)
    tiles = []
    for at in range(0, len(products), 16):
        tile = times_rows(curve, products[at : at + 16])
        for left, rows in ((weighted, lifted[at : at + 16]), (slope, sloped[at : at + 16])):
            if any(r is not None for r in rows):
                tile = tile + times_rows(left, [zero if r is None else r for r in rows])
        tiles.append(tile)
    sums = jnp.concatenate(tiles, axis=1)
    starts, size = row_starts(feats)
    corner = jnp.sum(weighted * ends, axis=1, keepdims=True)
    last = jnp.sum(slope * ends, axis=1, keepdims=True)
    last_at = starts[feats - 8] + feats - 1
    col = lax.broadcasted_iota(jnp.int32, (lines, size), 1)
    sums = sums + jnp.where(col == size - 1, corner, 0.0) + jnp.where(col == last_at, last, 0.0)
    if has_prev:
        sums = sums + prev_ref[...]
    sums_ref[...] = sums
    flow_ref[...] = flow
    ends_ref[...] = ends
    factor_ref[...] = factors


def penalty(own, got, per_line, policy_t, prev):
    lines, feats = policy_t.shape
    chunk = own.shape[1]
    size = row_starts(feats)[1]
    args = [own, got, per_line, policy_t] + ([] if prev is None else [prev])
    return pl.pallas_call(
        functools.partial(penalty_kernel, prev is not None),
        out_shape=[
            jax.ShapeDtypeStruct((lines, chunk), F32),
            jax.ShapeDtypeStruct((lines, chunk), F32),
            jax.ShapeDtypeStruct((feats, chunk), F32),
            jax.ShapeDtypeStruct((lines, size), F32),
        ],
        compiler_params=kernel_params(24),
        cost_estimate=cost(3e9, 4 * lines * (size * 2 + chunk * 6)),
        name="penalty",
    )(*args)


def solve_kernel(copies, lines, sums_ref, weight_ref, policy_ref, out_ref, rows_ref):
    feats = policy_ref.shape[0]
    starts, _ = row_starts(feats)
    total = sums_ref[0:lines]
    for src in range(1, copies):
        total = total + sums_ref[src * lines : (src + 1) * lines]
    square = jnp.concatenate([total, jnp.zeros((128 - lines, total.shape[1]), F32)], axis=0)
    weight = weight_ref[0:1]
    policy = policy_ref[...]
    margin = 1.0 - policy * policy
    diag = ridge_weight + barrier_weight * 2.0 * (1.0 + policy * policy) / (margin * margin)
    rows_ref[...] = square.T * weight
    sub = lax.broadcasted_iota(jnp.int32, (8, 128), 0)
    parts = []
    for q in range(feats // 8):
        top, next_row = starts[8 * q] + 8 * q, starts[8 * q + 1] + 8 * q
        parts.append(
            jnp.where(
                sub == 0, rows_ref[next_row + 7 : next_row + 8], rows_ref[top : top + 8]
            )
        )
    g = (
        jnp.concatenate(parts, axis=0)
        + ridge_weight * policy
        + barrier_weight * 2.0 * policy / margin
    )
    norm = jnp.sum(g * g, axis=0, keepdims=True)
    row = lax.broadcasted_iota(jnp.int32, (feats, 128), 0)
    for a in range(feats):
        at = starts[a] + 8 * (a // 8)
        rows_ref[at : at + 8] += jnp.where(sub == a % 8, diag[a : a + 1], 0.0)
    decrement = jnp.zeros((1, 128), F32)
    inverses = [None] * feats
    for c in reversed(range(feats)):
        height = 8 * row_blocks(c)
        pivot = rows_ref[starts[c] : starts[c] + height]
        inverse = 1.0 / pivot[c : c + 1]
        inverses[c] = inverse
        g_c = g[c : c + 1]
        decrement = decrement + g_c * g_c * inverse
        scaled = pivot * inverse
        for i in range(c):
            tall = 8 * row_blocks(i)
            rows_ref[starts[i] : starts[i] + tall] -= scaled[i : i + 1] * pivot[0:tall]
        full = scaled
        if height < feats:
            full = jnp.concatenate([scaled, jnp.zeros((feats - height, 128), F32)], axis=0)
        g = g - jnp.where(row < c, full * g_c, 0.0)
    x = jnp.zeros((feats, 128), F32)
    for i in range(feats):
        height = 8 * row_blocks(i)
        known = jnp.sum(
            rows_ref[starts[i] : starts[i] + height] * x[0:height], axis=0, keepdims=True
        )
        x_i = (g[i : i + 1] - known) * inverses[i]
        x = jnp.where(row == i, x_i, x)
    tail = jnp.concatenate([decrement, norm, jnp.zeros((128 - feats - 2, 128), F32)], axis=0)
    result = jnp.concatenate([-x, tail], axis=0).T[0:lines]
    for dst in range(copies):
        out_ref[dst * lines : (dst + 1) * lines] = result


def solve(sums, weight, policy_part, copies):
    lines = sums.shape[0] // copies
    return pl.pallas_call(
        functools.partial(solve_kernel, copies, lines),
        out_shape=jax.ShapeDtypeStruct((copies * lines, 128), F32),
        scratch_shapes=[pltpu.VMEM((sums.shape[1], 128), F32)],
        compiler_params=kernel_params(16),
        cost_estimate=cost(1e9, 4 * sums.size),
        name="solve",
    )(sums, weight, policy_part)


def tally_kernel(step_ref, out_ref):
    out_ref[...] = jnp.broadcast_to(jnp.sum(step_ref[...], axis=0, keepdims=True), out_ref.shape)


def tally(step, groups):
    return pl.pallas_call(
        tally_kernel,
        out_shape=jax.ShapeDtypeStruct((8 * groups, 128), F32),
        compiler_params=kernel_params(8),
        name="tally",
    )(step)


def shift_kernel(n, step_ref, *refs):
    flows, ends, factors = refs[:n], refs[n : 2 * n], refs[2 * n : 3 * n]
    flow_ref, shift_ref = refs[3 * n :]
    feats, chunk = factors[0].shape
    step = step_ref[...]
    for j in range(n):
        shift = (
            jnp.dot(step[:, 0:feats], factors[j][...], precision=HIGHEST, preferred_element_type=F32)
            + step[:, feats - 1 : feats] * ends[j][...]
        )
        shift_ref[j * chunk : (j + 1) * chunk] = shift.T
        flow_ref[j * chunk : (j + 1) * chunk] = flows[j][...].T


def shift_flows(step, flows, ends, factors):
    n = len(flows)
    lines, chunk = flows[0].shape
    out = jax.ShapeDtypeStruct((n * chunk, lines), F32)
    return pl.pallas_call(
        functools.partial(shift_kernel, n),
        out_shape=[out, out],
        compiler_params=kernel_params(16),
        cost_estimate=cost(3e9, 4 * n * chunk * lines * 4),
        name="shift",
    )(step, *flows, *ends, *factors)


def finish_kernel(entries, tally_ref, step_ref, policy_ref, flow_ref, shift_ref, *outs):
    policy_out, flow_out, decrement_out, norm_out = outs
    feats = policy_ref.shape[0]
    groups = tally_ref.shape[0] // 8
    total = tally_ref[0:1]
    for j in range(1, groups):
        total = total + tally_ref[8 * j : 8 * j + 1]
    root = jnp.sqrt(total)
    length = 1.0 / (1.0 + jnp.sqrt(total[:, feats : feats + 1] / (barrier_weight * entries)))
    policy_out[...] = policy_ref[...] + length * step_ref[...].T[0:feats]
    flow_out[...] = flow_ref[...] + length * shift_ref[...]
    decrement_out[...] = root[:, feats : feats + 1]
    norm_out[...] = root[:, feats + 1 : feats + 2]


def finish(entries, tallies, step, policy, flow, shift):
    one = jax.ShapeDtypeStruct((1, 1), F32)
    return pl.pallas_call(
        functools.partial(finish_kernel, entries),
        out_shape=[
            jax.ShapeDtypeStruct(policy.shape, F32),
            jax.ShapeDtypeStruct(flow.shape, F32),
            one,
            one,
        ],
        compiler_params=kernel_params(16),
        cost_estimate=cost(1e9, 12 * flow.size),
        name="finish",
    )(tallies, step, policy, flow, shift)


def swap(a, axis):
    return lax.ppermute(a, axis, [(0, 1), (1, 0)])


def step_on_shards(
    wind_dev, ptdf, region_weights, incidence, monitored, ratings, base_flow, line_cost, policy
):
    zs, ys = lax.axis_size("line_0"), lax.axis_size("line_1")
    z, y, core = lax.axis_index("line_0"), lax.axis_index("line_1"), lax.axis_index("sample_2")
    assert ys == 2 and zs % 2 == 0
    scen_here, width = wind_dev.shape
    lines_here = ptdf.shape[0]
    features = policy.shape[0]
    padded = -(-width // 128) * 128
    groups = scen_here // CHUNK
    up_ring = [(i, (i + 1) % zs) for i in range(zs)]
    down_ring = [(i, (i - 1) % zs) for i in range(zs)]

    wind = wind_dev.T
    chunks = [wind[:, j * CHUNK : (j + 1) * CHUNK] for j in range(groups)]
    half = lines_here // 2
    outgoing = repack(ptdf.T, True, 1 - y, core, half, zs, width, padded)
    part_a = swap(outgoing, "line_1")
    part_b = swap(part_a, "sample_2")
    endpoints = jnp.stack(
        [jnp.take(incidence[:, 0], monitored), jnp.take(incidence[:, 1], monitored)], axis=1
    )
    rating = jnp.take(ratings, monitored)

    assert zs == BLOCKS
    gathered = []
    for j, own in enumerate(chunks):
        pieces, up, down = [own], own, own
        for _ in range(1, zs // 2):
            up = lax.ppermute(up, "line_0", up_ring)
            down = lax.ppermute(down, "line_0", down_ring)
            pieces += [up, down]
        if j % 2 == 0:
            pieces.append(lax.ppermute(up, "line_0", up_ring))
        else:
            pieces.append(lax.ppermute(down, "line_0", down_ring))
        gathered.append(pieces)

    own_ptdf = repack(ptdf.T, True, y, 0, lines_here, zs, width, padded)
    region = repack(region_weights, False, y, 0, features, zs, width, padded)
    ends = ends_blocks(endpoints, y, zs, width, padded)
    part_points = swap(endpoints, "line_1")
    part_ends = ends_blocks(part_points, y, zs, width, padded)
    rhs = (own_ptdf, ends, region, part_a, part_b, part_ends)

    order = [0]
    for t in range(1, zs // 2):
        order += [-t, t]
    order.append(zs // 2)
    meta = jnp.stack([(z + t) % zs for t in order] + [core]).astype(jnp.int32)
    per_line = jnp.stack([base_flow, rating], axis=1)
    policy_t = policy.T
    flows, all_ends, factors, sums = [], [], [], None
    for pieces in gathered:
        early = partial_flows(meta, pieces[:-1], rhs, padded, None)
        own, send = partial_flows(meta, pieces[-1:], rhs, padded, early)
        got = swap(send, "line_1")
        flow, end, factor, sums = penalty(own, got, per_line, policy_t, sums)
        flows.append(flow)
        all_ends.append(end)
        factors.append(factor)

    copies = lax.axis_size(SAMPLE)
    share = lines_here // copies
    sums = lax.all_to_all(sums, SAMPLE, split_axis=0, concat_axis=0, tiled=True)
    at = lax.axis_index(SAMPLE) * share
    policy_part = jnp.pad(
        lax.dynamic_slice_in_dim(policy, at, share, 1), ((0, 0), (0, 128 - share))
    )
    weight = lax.dynamic_slice_in_dim(line_cost, at, share, 0) / (scen_here * copies)
    weight = jnp.broadcast_to(jnp.pad(weight, (0, 128 - share))[None, :], (8, 128))
    step = solve(sums, weight, policy_part, copies)
    step = lax.all_to_all(step, SAMPLE, split_axis=0, concat_axis=0, tiled=True)
    lines_axis = lax.axis_size(LINE)
    tallies = lax.all_to_all(
        tally(step, lines_axis), LINE, split_axis=0, concat_axis=0, tiled=True
    )
    flow, shift = shift_flows(step, flows, all_ends, factors)
    entries = features * lines_here * lines_axis
    new_policy, new_flows, decrement, norm = finish(entries, tallies, step, policy, flow, shift)
    return (new_policy, new_flows, decrement[0, 0], norm[0, 0])


def solution(mesh):
    torus = Mesh(
        mesh.devices.reshape(2, 4, 2, 8, 2),
        ("sample_0", "sample_1", "sample_2", "line_0", "line_1"),
    )
    return jax.shard_map(
        step_on_shards,
        mesh=torus,
        in_specs=(
            P(SAMPLE, LINE),
            P(LINE, None),
            P(),
            P(),
            P(LINE),
            P(),
            P(LINE),
            P(LINE),
            P(None, LINE),
        ),
        out_specs=(P(None, LINE), P(SAMPLE, LINE), P(), P()),
        check_vma=False,
    )
```
